1024 devices in a mesh: ep: 32 (over y, x, core), tp: 32 (over z).
Axes of the slice: x: 4, y: 4, z: 32, core: 2. Of those that a mesh axis runs over, the one named last changes fastest.
Arguments:
- tokens: bfloat16 [4096, 2048], P('ep', 'tp'), may hold values from -6 to 6
- routing: int32 [4096, 8], P('ep'), may hold values from 0 to 127, all different within a row; in each aligned block of 128 rows (0 to 127, 128 to 255, ...) at most 16 rows name the same one
- gate_fixed: int32 [4096, 8], P('ep'), may hold values from 1 to 65535
- gate_weight: bfloat16 [128, 2048, 768], P('ep', 'tp'), may hold values from -0.125 to 0.125
- up_weight: bfloat16 [128, 2048, 768], P('ep', 'tp'), may hold values from -0.25 to 0.25
- down_weight: bfloat16 [128, 2048, 768], P('ep', 'tp'), may hold values from -0.21875 to 0.21875
Outputs:
- layer_out: bfloat16 [4096, 2048], P('ep', 'tp')
The draws below stay inside these ranges and needn't reach their ends.
Inputs may be any that keep to these rules, and one draw needn't show every extreme that they name: `routing`: each token names 8 different experts. In each aligned block of 128 tokens (the tokens of one index of ep) no expert is named by more than 16 tokens, and in some blocks one expert is named by exactly 16.
All inputs are finite; a program needn't handle non-finite values.
Results may differ from the reference program's by a relative error of at most 0.0057.
Values may be sent and summed in bfloat16 or wider, within the bound.
No kernel may reach another device: no remote copies, remote signals or barrier semaphores. Data moves between devices by JAX's collectives and lax.ppermute only.
A program may use at most 64 MiB of HBM per device.

```python
import math
import jax
import jax.numpy as jnp
import numpy as np
from jax import lax

D = 2048
FF = 768
TOP = 8
TOK_EP = 128
EXPERTS = 128
CAP = 16
TOKENS = 4096
N_EP = 32


def set_ends(result, stream_key, smallest, high):
    extent = result.shape
    place = [jax.random.randint(jax.random.fold_in(stream_key, axis), (), 0, extent[axis]) for axis in range(len(extent))]
    result = result.at[tuple(place)].set(smallest)
    longest = extent.index(max(extent))
    place[longest] = (place[longest] + 1) % extent[longest]
    return result.at[tuple(place)].set(high)


def raised(drawn, stream_key, source, target, shards_of, factor):
    def block_of(dim):
        return (jnp.arange(drawn.shape[dim]) // (drawn.shape[dim] // shards_of)).reshape((-1,) + (1,) * (drawn.ndim - 1 - dim))

    near = jax.random.permutation(stream_key, shards_of)[block_of(target)]
    other_side = (block_of(target) + shards_of // 2) % shards_of
    return jnp.where((block_of(source) == near) | (block_of(source) == other_side), factor * drawn, drawn)


def shard_levels(stream_key, dims, cuts, least, top_value):
    loudness = 1.0
    for axis_at, shards_of in cuts:
        heights = jax.random.uniform(jax.random.fold_in(jax.random.fold_in(stream_key, 6), axis_at), (shards_of,), jnp.float32, least / len(cuts), top_value / len(cuts))
        loudness = loudness * jnp.repeat(jnp.exp(heights), dims[axis_at] // shards_of).reshape((-1,) + (1,) * (len(dims) - 1 - axis_at))
    return loudness


def shared_out(stream_key, own, number, rows, number_of, top, most, lean):
    ranking = jax.random.permutation(stream_key, number_of)
    packed, usual = load_shares(number_of, rows * top, most, lean, True), load_shares(number_of, rows * top, most, lean, False)
    places = jnp.arange(number_of)

    def named(tallies, rotation):
        used = int((tallies > 0).sum())
        fixed = max(1, used // 4)
        passed = fixed + (places - fixed + rotation * (used - fixed)) % max(1, number_of - fixed)
        return jnp.zeros((number_of,), jnp.int32).at[ranking[jnp.where(places < fixed, places, passed)]].set(jnp.asarray(tallies, jnp.int32))

    tallies = jnp.where(number % 4 == 0, named(packed, number // 4), named(usual, number - number // 4 - 1))
    mixed = jax.random.permutation(jax.random.fold_in(own, 3), number_of)
    source_of, taker = mixed[0:number_of // 2 * 2:2], mixed[1:number_of // 2 * 2:2]
    slack = jnp.minimum(tallies[source_of] - 1, most - tallies[taker]) // 2
    slack = jnp.where((source_of == ranking[0]) | (taker == ranking[0]) | (tallies[taker] == 0), 0, jnp.maximum(slack, 0))
    passed = jax.random.randint(jax.random.fold_in(own, 4), (number_of // 2,), 0, 1 << 20) % (slack + 1)
    tallies = tallies.at[source_of].add(-passed).at[taker].add(passed)
    members = jnp.searchsorted(jnp.cumsum(tallies), jnp.arange(rows * top), side="right").astype(jnp.int32)
    listing = members.reshape(top, rows).T
    listing = listing[jax.random.permutation(jax.random.fold_in(own, 1), rows)]
    rotation = jax.random.randint(jax.random.fold_in(own, 2), (rows, 1), 0, top)
    return jnp.take_along_axis(listing, (jnp.arange(top)[None, :] + rotation) % top, axis=1)


def load_shares(amount, total, most, skew, full):
    loads = [(1 << 20) // math.isqrt(standing ** skew) + 1 for standing in range(1, amount + 1)]
    largest = most if full else min(most, max(-(-total // amount), total * loads[0] // sum(loads)))
    least = 1 if total - largest >= amount - 1 else 0
    holding, spare = [largest] + [least] * (amount - 1), total - largest - least * (amount - 1)
    while spare > 0:
        free = [i for i in range(1, amount) if holding[i] < largest] or [i for i in range(1, amount) if holding[i] < most]
        mass, budget = sum([loads[i] for i in free]), spare
        for i in free:
            addition = min(most - holding[i], max(1, budget * loads[i] // mass), spare)
            holding[i] = holding[i] + addition
            spare = spare - addition
    return np.array(holding)


def centred(stream_key, shape, deviation, bound, shards=(), kind=jnp.bfloat16):
    level = shard_levels(stream_key, shape, shards, -0.22, 0.18) if shards else 1.0
    entries = jax.random.normal(stream_key, shape, jnp.float32) * deviation * level
    return jnp.minimum(jnp.maximum(entries, -bound), bound).astype(kind)


def gaussian_with(rng, shape, spread, limit, shards, heavy, kind=jnp.bfloat16):
    entries = spread * jax.random.normal(rng, shape, jnp.float32)
    if shards:
        entries = entries * shard_levels(rng, shape, shards, -0.22, 0.18)
    return jnp.clip(raised(entries, jax.random.fold_in(rng, 3), *heavy), -limit, limit).astype(kind)


def setup_inputs(seed: int = 0) -> dict:
    streams_of = jax.random.split(jax.random.key(seed), 7)
    tokens = centred(streams_of[0], (TOKENS, D), 1.0, 6.0, ((0, 32), (1, 32)))
    routing_keys = jax.random.split(jax.random.fold_in(streams_of[1], 1), TOKENS // TOK_EP)
    routing_turns = jax.random.permutation(jax.random.fold_in(streams_of[1], 3), TOKENS // TOK_EP)
    routing = jax.vmap(lambda own, number: shared_out(jax.random.fold_in(streams_of[1], 2), own, number, TOK_EP, EXPERTS, TOP, CAP, 1))(routing_keys, routing_turns).reshape((TOKENS, TOP))
    gate_fixed = set_ends(jax.random.randint(streams_of[2], (TOKENS, TOP), 1, 65536), jax.random.fold_in(streams_of[2], 1), 1, 65535).astype(jnp.int32)
    gate_weight = centred(streams_of[3], (EXPERTS, D, FF), D ** -0.5, 0.125, ((0, 32), (1, 32)))
    up_weight = gaussian_with(streams_of[4], (EXPERTS, D, FF), D ** -0.5, 0.25, ((0, 32), (1, 32)), (1, 2, 32, 2.75))
    down_weight = centred(streams_of[5], (EXPERTS, D, FF), FF ** -0.5, 0.21875, ((0, 32), (1, 32)))
    return dict(tokens=tokens, routing=routing, gate_fixed=gate_fixed, gate_weight=gate_weight, up_weight=up_weight, down_weight=down_weight)


def slot_positions(block_ids, experts):
    one_hot = (block_ids[..., None] == jnp.arange(experts, dtype=jnp.int32)).astype(jnp.int32)
    earlier = jnp.cumsum(one_hot, axis=1) - one_hot
    return jnp.sum(earlier * one_hot, axis=-1).astype(jnp.int32)


def expert_step(operands):
    slot_rows, gate_mat, up_mat, down_mat = operands
    gate_acts = jnp.dot(slot_rows, gate_mat, preferred_element_type=jnp.float32)
    up_acts = jnp.dot(slot_rows, up_mat, preferred_element_type=jnp.float32)
    hidden = (jax.nn.silu(gate_acts) * up_acts).astype(jnp.bfloat16)
    return jnp.dot(hidden, down_mat.T, preferred_element_type=jnp.float32).astype(jnp.bfloat16)


def reference(tokens, routing, gate_fixed, gate_weight, up_weight, down_weight):
    block_ids = routing.reshape(N_EP, TOK_EP * TOP).astype(jnp.int32)
    position = slot_positions(block_ids, EXPERTS)
    block_iota = jnp.broadcast_to(jnp.arange(N_EP, dtype=jnp.int32)[:, None], block_ids.shape)
    copies = jnp.repeat(tokens, TOP, axis=0).reshape(N_EP, TOK_EP * TOP, D)
    slot_rows = jnp.zeros((EXPERTS, N_EP, CAP, D), jnp.bfloat16)
    slot_rows = slot_rows.at[block_ids, block_iota, position].set(copies)
    results = lax.map(expert_step, (slot_rows.reshape(EXPERTS, N_EP * CAP, D), gate_weight, up_weight, down_weight))
    picked = results.reshape(EXPERTS, N_EP, CAP, D)[block_ids, block_iota, position]
    scales = (gate_fixed.astype(jnp.float32) / 65536.0).reshape(N_EP, TOK_EP * TOP, 1)
    mixed = (picked.astype(jnp.float32) * scales).reshape(TOKENS, TOP, D)
    return jnp.sum(mixed, axis=1).astype(jnp.bfloat16)
```

```python
import jax
import jax.numpy as jnp
from jax import lax
from jax.sharding import PartitionSpec as P

F32 = jnp.float32
BF16 = jnp.bfloat16


def exchange(x, axis, groups=None):
    return lax.all_to_all(
        x, axis, split_axis=0, concat_axis=0, tiled=True, axis_index_groups=groups
    )


def by_position(w, halves):
    e, f, u = w.shape
    return w.reshape(e, f, halves, u // halves).transpose(0, 2, 1, 3).reshape(
        e * halves, f, u // halves
    )


def on_device(tokens, routing, gate_fixed, gate_weight, up_weight, down_weight):
    ep = lax.axis_size("ep")
    tp = lax.axis_size("tp")
    local, share, hidden_width = gate_weight.shape
    rows, top = routing.shape
    capacity = max(2, rows * top * 2 // (local * ep))
    spread = 4
    members = tp // spread
    halves = members // local
    units = hidden_width // halves
    slots = ep * capacity
    far = [[j * spread + r for j in range(members)] for r in range(spread)]
    near = [[i * spread + r for r in range(spread)] for i in range(members)]
    z = lax.axis_index("tp")
    mine = z // (spread * halves)
    me = z % spread

    w_in = jnp.concatenate(
        [by_position(gate_weight, halves), by_position(up_weight, halves)], axis=2
    )
    w_gu = exchange(w_in, "tp", far).reshape(members * share, 2 * units)
    w_down = exchange(by_position(down_weight, halves), "tp", far).reshape(
        members * share, units
    )

    xt = exchange(
        jnp.broadcast_to(tokens.T[None], (members, share, rows)), "tp", far
    ).reshape(members * share, rows)

    rt = routing.T
    expert = jnp.arange(ep, dtype=jnp.int32) * local + mine
    hit = rt[:, None, :] == expert[None, :, None]
    named = jnp.any(hit, axis=0)
    scale = jnp.sum(jnp.where(hit, gate_fixed.T[:, None, :], 0), axis=0)
    t = jnp.arange(rows)
    before = (t[:, None] < t[None, :]).astype(BF16)
    position = jnp.dot(named.astype(BF16), before, preferred_element_type=F32)
    slot = jnp.arange(capacity).astype(F32)[None, :, None]
    pick = named[:, None, :] & (position[:, None, :] == slot)
    place = pick.astype(BF16).reshape(slots, rows)
    high = (scale >> 8).astype(F32) / 256.0
    low = (scale & 255).astype(F32) / 65536.0
    mix_high = jnp.where(pick, high[:, None, :], 0.0).astype(BF16).reshape(slots, rows)
    mix_low = jnp.where(pick, low[:, None, :], 0.0).astype(BF16).reshape(slots, rows)

    outgoing = lax.dot_general(
        place, xt, (((1,), (1,)), ((), ())), preferred_element_type=F32
    ).astype(BF16)
    x = exchange(outgoing.reshape(ep, capacity, -1), "ep").reshape(slots, -1)

    part = jnp.dot(x, w_gu, preferred_element_type=F32).reshape(
        spread, slots // spread, 2 * units
    )
    others = exchange(part.astype(BF16), "tp", near).astype(F32)
    own = lax.dynamic_index_in_dim(part, me, 0, keepdims=False)
    keep = (jnp.arange(spread) != me)[:, None, None]
    acts = own + jnp.sum(jnp.where(keep, others, 0.0), axis=0)
    share_hidden = (jax.nn.silu(acts[:, :units]) * acts[:, units:]).astype(BF16)
    hidden = exchange(
        jnp.broadcast_to(share_hidden[None], (spread,) + share_hidden.shape), "tp", near
    ).reshape(slots, units)
    result = lax.dot_general(
        hidden, w_down, (((1,), (1,)), ((), ())), preferred_element_type=F32
    ).astype(BF16)
    back = exchange(result.reshape(ep, capacity, -1), "ep").reshape(slots, -1)

    over_slots = (((0,), (0,)), ((), ()))
    mixed = lax.dot_general(
        back, mix_high, over_slots, preferred_element_type=F32
    ) + lax.dot_general(back, mix_low, over_slots, preferred_element_type=F32)
    mixed = mixed.reshape(members, share, rows)
    parts = exchange(mixed.astype(BF16), "tp", far)
    out = jnp.sum(parts.astype(F32), axis=0).astype(BF16)
    return out.T


def solution(mesh):
    in_specs = (
        P("ep", "tp"),
        P("ep", None),
        P("ep", None),
        P("ep", "tp", None),
        P("ep", "tp", None),
        P("ep", "tp", None),
    )
    return jax.shard_map(
        on_device, mesh=mesh, in_specs=in_specs, out_specs=P("ep", "tp"), check_vma=False
    )
```

```python
import jax
import jax.numpy as jnp
from jax import lax
from jax.sharding import PartitionSpec as P

F32 = jnp.float32
BF16 = jnp.bfloat16


def exchange(x, axis, groups=None):
    return lax.all_to_all(
        x, axis, split_axis=0, concat_axis=0, tiled=True, axis_index_groups=groups
    )


def turned(x, amount):
    n = x.shape[0]
    return lax.dynamic_slice_in_dim(jnp.concatenate([x, x], axis=0), amount, n, axis=0)


def on_device(tokens, routing, gate_fixed, gate_weight, up_weight, down_weight):
    ep = lax.axis_size("ep")
    tp = lax.axis_size("tp")
    local, share, units = gate_weight.shape
    rows, top = routing.shape
    capacity = max(2, rows * top * 2 // (local * ep))
    ring = tp // local
    half = ring // 2
    slots = ep * capacity
    chunk = slots // ring
    cut = chunk // 2
    near = [[p * local + r for r in range(local)] for p in range(ring)]
    z = lax.axis_index("tp")
    me = lax.rem(z, local)
    here = lax.div(z, local)

    def along(x, step):
        return lax.ppermute(
            x, "tp", [(i, (i + step * local) % tp) for i in range(tp)]
        )

    def beside(x, k):
        return lax.ppermute(
            x, "tp", [(g[i], g[(i + k) % local]) for g in near for i in range(local)]
        )

    def weight_block(k):
        e = lax.rem(me + k, local)
        return jnp.concatenate(
            [
                lax.dynamic_index_in_dim(w, e, 0, keepdims=False)
                for w in (gate_weight, up_weight, down_weight)
            ],
            axis=1,
        )

    blocks = [weight_block(0)] + [beside(weight_block(k), k) for k in range(1, local)]
    w_gu = jnp.concatenate([b[:, : 2 * units] for b in blocks], axis=0)
    w_down = jnp.concatenate([b[:, 2 * units :] for b in blocks], axis=0)

    xt = exchange(jnp.broadcast_to(tokens.T[None], (local, share, rows)), "tp", near)
    order = [lax.rem(me - k + local, local) for k in range(local)]
    xt = jnp.concatenate(
        [lax.dynamic_index_in_dim(xt, o, 0, keepdims=False) for o in order], axis=0
    )

    rt = routing.T
    expert = jnp.arange(ep, dtype=jnp.int32) * local + me
    hit = rt[:, None, :] == expert[None, :, None]
    named = jnp.any(hit, axis=0)
    scale = jnp.sum(jnp.where(hit, gate_fixed.T[:, None, :], 0), axis=0)
    t = jnp.arange(rows)
    before = (t[:, None] < t[None, :]).astype(BF16)
    position = jnp.dot(named.astype(BF16), before, preferred_element_type=F32)
    slot = jnp.arange(capacity).astype(F32)[None, :, None]
    pick = named[:, None, :] & (position[:, None, :] == slot)
    place = pick.astype(BF16).reshape(slots, rows)
    factor = scale.astype(F32) / 65536.0
    mix = jnp.where(pick, factor[:, None, :], 0.0).reshape(slots, rows)

    outgoing = lax.dot_general(
        place, xt, (((1,), (1,)), ((), ())), preferred_element_type=F32
    ).astype(BF16)
    x = exchange(outgoing.reshape(ep, capacity, -1), "ep")

    x = turned(x.reshape(ring, chunk, -1), here).reshape(slots, -1)
    part = jnp.dot(x, w_gu, preferred_element_type=F32).reshape(ring, chunk, 2 * units)
    plus = along(part[half, :cut].astype(BF16), 1)
    minus = along(part[half, cut:].astype(BF16), -1)
    for k in range(half - 1, 0, -1):
        up, down = part[k], part[ring - k]
        if k == half - 1:
            up = jnp.concatenate([up[:cut] + plus.astype(F32), up[cut:]], axis=0)
            down = jnp.concatenate([down[:cut], down[cut:] + minus.astype(F32)], axis=0)
        else:
            up = up + plus.astype(F32)
            down = down + minus.astype(F32)
        plus = along(up.astype(BF16), 1)
        minus = along(down.astype(BF16), -1)
    acts = part[0] + (plus.astype(F32) + minus.astype(F32))
    own = (jax.nn.silu(acts[:, :units]) * acts[:, units:]).astype(BF16)

    hidden = [own] + [None] * (ring - 1)
    left = right = own
    for k in range(1, half):
        left, right = along(left, 1), along(right, -1)
        hidden[ring - k], hidden[k] = left, right
    hidden[half] = jnp.concatenate([along(left[:cut], 1), along(right[cut:], -1)], axis=0)
    result = lax.dot_general(
        jnp.concatenate(hidden, axis=0),
        w_down,
        (((1,), (1,)), ((), ())),
        preferred_element_type=F32,
    )
    result = turned(result.reshape(ring, chunk, -1), lax.rem(ring - here, ring))
    back = exchange(result.reshape(ep, capacity, -1), "ep").reshape(slots, -1)

    mixed = lax.dot_general(
        back,
        mix,
        (((0,), (0,)), ((), ())),
        precision=lax.Precision.HIGHEST,
        preferred_element_type=F32,
    ).reshape(local, share, rows)
    mixed = jnp.stack([lax.dynamic_index_in_dim(mixed, o, 0, keepdims=False) for o in order])
    parts = exchange(mixed, "tp", near)
    return jnp.sum(parts, axis=0).astype(BF16).T


def solution(mesh):
    in_specs = (
        P("ep", "tp"),
        P("ep", None),
        P("ep", None),
        P("ep", "tp", None),
        P("ep", "tp", None),
        P("ep", "tp", None),
    )
    return jax.shard_map(
        on_device, mesh=mesh, in_specs=in_specs, out_specs=P("ep", "tp"), check_vma=False
    )
```

```python
import jax
import jax.numpy as jnp
from jax import lax
from jax.sharding import PartitionSpec as P

F32 = jnp.float32
BF16 = jnp.bfloat16


def exchange(x, axis, groups=None):
    return lax.all_to_all(
        x, axis, split_axis=0, concat_axis=0, tiled=True, axis_index_groups=groups
    )


def picked(x, places):
    return [lax.dynamic_index_in_dim(x, i, 0, keepdims=False) for i in places]


def rows_dot(a, b):
    return lax.dot_general(a, b, (((1,), (1,)), ((), ())), preferred_element_type=F32)


def on_device(tokens, routing, gate_fixed, gate_weight, up_weight, down_weight):
    ep = lax.axis_size("ep")
    tp = lax.axis_size("tp")
    local, share, units = gate_weight.shape
    rows, top = routing.shape
    capacity = max(2, rows * top * 2 // (local * ep))
    ring = tp // local
    slots = ep * capacity
    chunk = slots // ring
    part_units = units // 2
    near = [[p * local + r for r in range(local)] for p in range(ring)]
    z = lax.axis_index("tp")
    me = lax.rem(z, local)
    here = lax.div(z, local)

    def sign_of(p, r):
        return 1 if (p % 2 == 0) == (r < local // 2) else -1

    sign = jnp.where((lax.rem(here, 2) == 0) == (me < local // 2), 1, -1)

    def swap(x, side):
        pairs = [
            (p * local + r, (p + side * sign_of(p, r)) % ring * local + r)
            for p in range(ring)
            for r in range(local)
        ]
        return lax.ppermute(x, "tp", pairs)

    def beside(x, k):
        return lax.ppermute(
            x, "tp", [(g[i], g[(i + k) % local]) for g in near for i in range(local)]
        )

    chunk_at = [lax.rem(here + k * sign + ring, ring) for k in range(ring)]
    chunk_of = [lax.rem((c - here) * sign + 2 * ring, ring) for c in range(ring)]

    xt = exchange(jnp.broadcast_to(tokens.T[None], (local, share, rows)), "tp", near)
    order = [lax.rem(me - k + local, local) for k in range(local)]
    xt = jnp.concatenate(picked(xt, order), axis=0)

    def in_block(k):
        e = lax.rem(me + k, local)
        g = lax.dynamic_index_in_dim(gate_weight, e, 0, keepdims=False)
        u = lax.dynamic_index_in_dim(up_weight, e, 0, keepdims=False)
        return jnp.concatenate(
            [g[:, :part_units], u[:, :part_units], g[:, part_units:], u[:, part_units:]],
            axis=1,
        )

    def down_block(k):
        return lax.dynamic_index_in_dim(
            down_weight, lax.rem(me + k, local), 0, keepdims=False
        )

    w_in = [in_block(0)] + [beside(in_block(k), k) for k in range(1, local)]

    rt = routing.T
    expert = jnp.arange(ep, dtype=jnp.int32) * local + me
    hit = rt[:, None, :] == expert[None, :, None]
    named = jnp.any(hit, axis=0)
    scale = jnp.sum(jnp.where(hit, gate_fixed.T[:, None, :], 0), axis=0)
    t = jnp.arange(rows)
    before = (t[:, None] < t[None, :]).astype(BF16)
    position = jnp.dot(named.astype(BF16), before, preferred_element_type=F32)
    slot = jnp.arange(capacity).astype(F32)[None, :, None]
    pick = named[:, None, :] & (position[:, None, :] == slot)
    place = pick.astype(BF16).reshape(slots, rows)
    factor = scale.astype(F32) / 65536.0
    mix = jnp.where(pick, factor[:, None, :], 0.0).reshape(slots, rows)

    outgoing = rows_dot(place, xt).astype(BF16)
    sent = [down_block(k) for k in range(1, local)]
    outgoing, sent = lax.optimization_barrier((outgoing, sent))
    x = exchange(outgoing.reshape(ep, capacity, -1), "ep")
    w_down = [down_block(0)] + [beside(b, k + 1) for k, b in enumerate(sent)]
    w_down = jnp.concatenate(w_down, axis=0)

    x = jnp.concatenate(picked(x.reshape(ring, chunk, -1), chunk_at), axis=0)
    width = 2 * part_units
    streams = []
    for h in range(2):
        w = jnp.concatenate([b[:, h * width : (h + 1) * width] for b in w_in], axis=0)
        streams.append(
            jnp.dot(x, w, preferred_element_type=F32).reshape(ring, chunk, width)
        )

    def both(a, b):
        return jnp.stack([a, b]).astype(BF16)

    def summed(part):
        r = swap(both(part[5], part[4]), -1).astype(F32)
        yield
        r = swap(both(part[2] + r[0], part[3] + r[1]), 1).astype(F32)
        yield
        r = swap(both(part[7] + r[0], part[6] + r[1]), -1).astype(F32)
        yield
        r0, r1 = part[0] + r[0], part[1] + r[1]
        acts = r0 + swap(r1.astype(BF16), 1).astype(F32)
        own = jax.nn.silu(acts[:, :part_units]) * acts[:, part_units:]
        yield own.astype(BF16)

    def shared(own):
        first = jnp.stack([own, swap(own, 1)])
        yield
        second = swap(first, -1)
        yield
        third = swap(second, 1)
        yield
        fourth = swap(third, -1)
        yield [first[0], first[1], third[0], third[1], fourth[1], fourth[0], second[1], second[0]]

    def run(steps):
        value = None
        while True:
            got = []
            for s in steps:
                got.append(next(s))
            if got[0] is not None:
                return got

    own = run([summed(p) for p in streams])
    blocks = run([shared(o) for o in own])
    result = rows_dot(jnp.concatenate(blocks[0], axis=0), w_down[:, :part_units]) + rows_dot(
        jnp.concatenate(blocks[1], axis=0), w_down[:, part_units:]
    )
    result = jnp.concatenate(picked(result.reshape(ring, chunk, -1), chunk_of), axis=0)
    back = exchange(result.reshape(ep, capacity, -1), "ep").reshape(slots, -1)

    mixed = lax.dot_general(
        back,
        mix,
        (((0,), (0,)), ((), ())),
        precision=lax.Precision.HIGHEST,
        preferred_element_type=F32,
    ).reshape(local, share, rows)
    parts = exchange(jnp.stack(picked(mixed, order)), "tp", near)
    return jnp.sum(parts, axis=0).astype(BF16).T


def solution(mesh):
    in_specs = (
        P("ep", "tp"),
        P("ep", None),
        P("ep", None),
        P("ep", "tp", None),
        P("ep", "tp", None),
        P("ep", "tp", None),
    )
    return jax.shard_map(
        on_device, mesh=mesh, in_specs=in_specs, out_specs=P("ep", "tp"), check_vma=False
    )
```

```python
import jax
import jax.numpy as jnp
from jax import lax
from jax.sharding import PartitionSpec as P

F32 = jnp.float32
BF16 = jnp.bfloat16


def exchange(x, axis, groups=None):
    return lax.all_to_all(
        x, axis, split_axis=0, concat_axis=0, tiled=True, axis_index_groups=groups
    )


def picked(x, places):
    return [lax.dynamic_index_in_dim(x, i, 0, keepdims=False) for i in places]


def rows_dot(a, b):
    return lax.dot_general(a, b, (((1,), (1,)), ((), ())), preferred_element_type=F32)


def layer(tokens, routing, gate_fixed, gate_weight, up_weight, down_weight):
    ep = lax.axis_size("ep")
    tp = lax.axis_size("tp")
    local, share, units = gate_weight.shape
    rows, top = routing.shape
    capacity = max(2, rows * top * 2 // (local * ep))
    ring = tp // local
    slots = ep * capacity
    chunk = slots // ring
    near = [[p * local + r for r in range(local)] for p in range(ring)]
    z = lax.axis_index("tp")
    me = lax.rem(z, local)
    here = lax.div(z, local)

    def sign_of(r):
        return 1 if r < local // 2 else -1

    sign = jnp.where(me < local // 2, 1, -1)

    def ship(x, side):
        pairs = [
            (p * local + r, (p + side * sign_of(r)) % ring * local + r)
            for p in range(ring)
            for r in range(local)
        ]
        return lax.ppermute(x, "tp", pairs)

    def beside(x, k):
        return lax.ppermute(
            x, "tp", [(g[i], g[(i + k) % local]) for g in near for i in range(local)]
        )

    chunk_at = [lax.rem(here + k * sign + ring, ring) for k in range(ring)]

    xt = exchange(jnp.broadcast_to(tokens.T[None], (local, share, rows)), "tp", near)
    order = [lax.rem(me - k + local, local) for k in range(local)]
    xt = jnp.concatenate(picked(xt, order), axis=0)

    def in_block(k):
        e = lax.rem(me + k, local)
        g = lax.dynamic_index_in_dim(gate_weight, e, 0, keepdims=False)
        u = lax.dynamic_index_in_dim(up_weight, e, 0, keepdims=False)
        return jnp.concatenate([g, u], axis=1)

    def down_block(k):
        return lax.dynamic_index_in_dim(
            down_weight, lax.rem(me + k, local), 0, keepdims=False
        )

    w_in = [in_block(0)] + [beside(in_block(k), k) for k in range(1, local)]

    rt = routing.T
    expert = jnp.arange(ep, dtype=jnp.int32) * local + me
    hit = rt[:, None, :] == expert[None, :, None]
    named = jnp.any(hit, axis=0)
    scale = jnp.sum(jnp.where(hit, gate_fixed.T[:, None, :], 0), axis=0)
    t = jnp.arange(rows)
    before = (t[:, None] < t[None, :]).astype(BF16)
    position = jnp.dot(named.astype(BF16), before, preferred_element_type=F32)
    slot = jnp.arange(capacity).astype(F32)[None, :, None]
    pick = named[:, None, :] & (position[:, None, :] == slot)
    place = pick.astype(BF16).reshape(slots, rows)
    factor = scale.astype(F32) / 65536.0
    mix = jnp.where(pick, factor[:, None, :], 0.0).reshape(slots, rows)

    outgoing = rows_dot(place, xt).astype(BF16)
    sent = [down_block(k) for k in range(1, local)]
    outgoing, sent = lax.optimization_barrier((outgoing, sent))
    x = exchange(outgoing.reshape(ep, capacity, -1), "ep")
    w_down = [down_block(0)] + [beside(b, k + 1) for k, b in enumerate(sent)]
    w_down = jnp.concatenate(w_down, axis=0)

    x = x.reshape(ring, chunk, -1)
    w_in = jnp.concatenate(w_in, axis=0)

    def term(k):
        rows_of = lax.dynamic_index_in_dim(x, chunk_at[k % ring], 0, keepdims=False)
        return jnp.dot(rows_of, w_in, preferred_element_type=F32)

    steps = ring // 2
    ahead = ship(term(steps).astype(BF16), 1)
    behind = ship(term(1 - steps).astype(BF16), -1)
    for k in range(steps - 1, 0, -1):
        ahead = ship((term(k) + ahead.astype(F32)).astype(BF16), 1)
        if k > 1:
            behind = ship((term(1 - k) + behind.astype(F32)).astype(BF16), -1)
    acts = term(0) + ahead.astype(F32) + behind.astype(F32)
    own = (jax.nn.silu(acts[:, :units]) * acts[:, units:]).astype(BF16)

    result = jnp.zeros((ring, chunk, local * share), F32)

    def put(result, hidden, k):
        return lax.dynamic_update_index_in_dim(
            result, rows_dot(hidden, w_down), chunk_at[k % ring], 0
        )

    ahead = behind = own
    result = put(result, own, 0)
    for k in range(1, steps + 1):
        ahead = ship(ahead, 1)
        result = put(result, ahead, -k)
        if k < steps:
            behind = ship(behind, -1)
            result = put(result, behind, k)
    back = exchange(result.reshape(ep, capacity, -1), "ep").reshape(slots, -1)

    mixed = lax.dot_general(
        back,
        mix,
        (((0,), (0,)), ((), ())),
        precision=lax.Precision.HIGHEST,
        preferred_element_type=F32,
    ).reshape(local, share, rows)
    parts = exchange(jnp.stack(picked(mixed, order)), "tp", near)
    return jnp.sum(parts, axis=0).astype(BF16).T


def solution(mesh):
    in_specs = (
        P("ep", "tp"),
        P("ep", None),
        P("ep", None),
        P("ep", "tp", None),
        P("ep", "tp", None),
        P("ep", "tp", None),
    )
    return jax.shard_map(
        layer, mesh=mesh, in_specs=in_specs, out_specs=P("ep", "tp"), check_vma=False
    )
```

```python
import jax
import jax.numpy as jnp
from jax import lax
from jax.sharding import PartitionSpec as P

F32 = jnp.float32
BF16 = jnp.bfloat16


def exchange(x, axis, groups=None):
    return lax.all_to_all(
        x, axis, split_axis=0, concat_axis=0, tiled=True, axis_index_groups=groups
    )


def picked(x, places):
    return [lax.dynamic_index_in_dim(x, i, 0, keepdims=False) for i in places]


def rows_dot(a, b):
    return lax.dot_general(a, b, (((1,), (1,)), ((), ())), preferred_element_type=F32)


def layer(tokens, routing, gate_fixed, gate_weight, up_weight, down_weight):
    ep = lax.axis_size("ep")
    tp = lax.axis_size("tp")
    local, share, units = gate_weight.shape
    rows, top = routing.shape
    capacity = max(2, rows * top * 2 // (local * ep))
    ring = tp // local
    slots = ep * capacity
    chunk = slots // ring
    near = [[p * local + r for r in range(local)] for p in range(ring)]
    z = lax.axis_index("tp")
    me = lax.rem(z, local)
    here = lax.div(z, local)

    def sign_of(r):
        return 1 if r < local // 2 else -1

    sign = jnp.where(me < local // 2, 1, -1)

    def ship(x, side):
        pairs = [
            (p * local + r, (p + side * sign_of(r)) % ring * local + r)
            for p in range(ring)
            for r in range(local)
        ]
        return lax.ppermute(x, "tp", pairs)

    def beside(x, k):
        return lax.ppermute(
            x, "tp", [(g[i], g[(i + k) % local]) for g in near for i in range(local)]
        )

    chunk_at = [lax.rem(here + k * sign + ring, ring) for k in range(ring)]

    xt = exchange(jnp.broadcast_to(tokens.T[None], (local, share, rows)), "tp", near)
    order = [lax.rem(me - k + local, local) for k in range(local)]
    xt = jnp.concatenate(picked(xt, order), axis=0)

    def in_block(k):
        e = lax.rem(me + k, local)
        g = lax.dynamic_index_in_dim(gate_weight, e, 0, keepdims=False)
        u = lax.dynamic_index_in_dim(up_weight, e, 0, keepdims=False)
        return jnp.concatenate([g, u], axis=1)

    def down_block(k):
        return lax.dynamic_index_in_dim(
            down_weight, lax.rem(me + k, local), 0, keepdims=False
        )

    w_in = [in_block(0)] + [beside(in_block(k), k) for k in range(1, local)]

    rt = routing.T
    expert = jnp.arange(ep, dtype=jnp.int32) * local + me
    hit = rt[:, None, :] == expert[None, :, None]
    named = jnp.any(hit, axis=0)
    t = jnp.arange(rows)
    before = (t[:, None] < t[None, :]).astype(BF16)
    position = jnp.dot(named.astype(BF16), before, preferred_element_type=F32)
    slot = jnp.arange(capacity).astype(F32)[None, :, None]
    pick = named[:, None, :] & (position[:, None, :] == slot)
    place = pick.astype(BF16).reshape(slots, rows)
    outgoing = rows_dot(place, xt).astype(BF16)
    sent = [down_block(k) for k in range(1, local)]
    outgoing, sent = lax.optimization_barrier((outgoing, sent))
    x = exchange(outgoing.reshape(ep, capacity, -1), "ep")
    w_down = [down_block(0)] + [beside(b, k + 1) for k, b in enumerate(sent)]
    w_down = jnp.stack(picked(jnp.stack(w_down), order))

    x = x.reshape(ring, chunk, -1)
    w_in = jnp.concatenate(w_in, axis=0)

    def term(k):
        rows_of = lax.dynamic_index_in_dim(x, chunk_at[k % ring], 0, keepdims=False)
        return jnp.dot(rows_of, w_in, preferred_element_type=F32)

    steps = ring // 2
    ahead = ship(term(steps).astype(BF16), 1)
    behind = ship(term(1 - steps).astype(BF16), -1)
    for k in range(steps - 1, 0, -1):
        ahead = ship((term(k) + ahead.astype(F32)).astype(BF16), 1)
        if k > 1:
            behind = ship((term(1 - k) + behind.astype(F32)).astype(BF16), -1)
    acts = term(0) + ahead.astype(F32) + behind.astype(F32)
    own = (jax.nn.silu(acts[:, :units]) * acts[:, units:]).astype(BF16)

    low = capacity // 2
    empty = jnp.zeros_like(w_down)
    w_down = jnp.stack(
        [jnp.concatenate([w_down, empty], axis=2), jnp.concatenate([empty, w_down], axis=2)],
        axis=1,
    ).reshape(local * 2 * share, 2 * units)
    sources = chunk // capacity
    result = jnp.zeros((ring, sources, local, low, 2 * share), F32)

    def put(result, hidden, k):
        pair = hidden.reshape(sources, 2, low, units)
        pair = jnp.concatenate([pair[:, 0], pair[:, 1]], axis=2)
        tile = rows_dot(pair.reshape(sources * low, 2 * units), w_down)
        tile = tile.reshape(sources, low, local, 2 * share).transpose(0, 2, 1, 3)
        return lax.dynamic_update_index_in_dim(result, tile, chunk_at[k % ring], 0)

    ahead = behind = own
    result = put(result, own, 0)
    for k in range(1, steps + 1):
        ahead = ship(ahead, 1)
        result = put(result, ahead, -k)
        if k < steps:
            behind = ship(behind, -1)
            result = put(result, behind, k)

    groups = [
        [e * tp + p * local + r for e in range(ep) for r in range(local)] for p in range(ring)
    ]
    back = lax.all_to_all(
        result.reshape(ep * local, low, 2 * share),
        ("ep", "tp"),
        split_axis=0,
        concat_axis=0,
        tiled=True,
        axis_index_groups=groups,
    )

    each = jnp.arange(ep * local, dtype=jnp.int32)
    hit = rt[:, None, :] == each[None, :, None]
    named = jnp.any(hit, axis=0)
    scale = jnp.sum(jnp.where(hit, gate_fixed.T[:, None, :], 0), axis=0)
    position = jnp.dot(named.astype(BF16), before, preferred_element_type=F32)
    position = jnp.where(named, position, -1.0)[:, None, :]
    factor = (scale.astype(F32) / 65536.0)[:, None, :]
    slot = jnp.arange(low).astype(F32)[None, :, None]
    mix = jnp.concatenate(
        [
            jnp.where(position == slot, factor, 0.0),
            jnp.where(position == slot + low, factor, 0.0),
        ],
        axis=2,
    ).reshape(ep * local * low, 2 * rows)
    mixed = lax.dot_general(
        back.reshape(ep * local * low, 2 * share),
        mix,
        (((0,), (0,)), ((), ())),
        precision=lax.Precision.HIGHEST,
        preferred_element_type=F32,
    )
    return (mixed[:share, :rows] + mixed[share:, rows:]).astype(BF16).T


def solution(mesh):
    in_specs = (
        P("ep", "tp"),
        P("ep", None),
        P("ep", None),
        P("ep", "tp", None),
        P("ep", "tp", None),
        P("ep", "tp", None),
    )
    return jax.shard_map(
        layer, mesh=mesh, in_specs=in_specs, out_specs=P("ep", "tp"), check_vma=False
    )
```

```python
import jax
import jax.numpy as jnp
from jax import lax
from jax.sharding import PartitionSpec as P

F32 = jnp.float32
BF16 = jnp.bfloat16


def exchange(x, axis, groups=None):
    return lax.all_to_all(
        x, axis, split_axis=0, concat_axis=0, tiled=True, axis_index_groups=groups
    )


def picked(x, places):
    return [lax.dynamic_index_in_dim(x, i, 0, keepdims=False) for i in places]


def rows_dot(a, b):
    return lax.dot_general(a, b, (((1,), (1,)), ((), ())), preferred_element_type=F32)


def layer(tokens, routing, gate_fixed, gate_weight, up_weight, down_weight):
    ep = lax.axis_size("ep")
    tp = lax.axis_size("tp")
    local, share, units = gate_weight.shape
    rows, top = routing.shape
    capacity = max(2, rows * top * 2 // (local * ep))
    ring = tp // local
    slots = ep * capacity
    chunk = slots // ring
    near = [[p * local + r for r in range(local)] for p in range(ring)]
    z = lax.axis_index("tp")
    me = lax.rem(z, local)
    here = lax.div(z, local)

    def sign_of(r):
        return 1 if r < local // 2 else -1

    sign = jnp.where(me < local // 2, 1, -1)

    def ship(x, side):
        pairs = [
            (p * local + r, (p + side * sign_of(r)) % ring * local + r)
            for p in range(ring)
            for r in range(local)
        ]
        return lax.ppermute(x, "tp", pairs)

    def beside(x, k):
        return lax.ppermute(
            x, "tp", [(g[i], g[(i + k) % local]) for g in near for i in range(local)]
        )

    chunk_at = [lax.rem(here + k * sign + ring, ring) for k in range(ring)]

    xt = exchange(jnp.broadcast_to(tokens.T[None], (local, share, rows)), "tp", near)
    order = [lax.rem(me - k + local, local) for k in range(local)]
    xt = jnp.concatenate(picked(xt, order), axis=0)

    def in_block(k):
        e = lax.rem(me + k, local)
        g = lax.dynamic_index_in_dim(gate_weight, e, 0, keepdims=False)
        u = lax.dynamic_index_in_dim(up_weight, e, 0, keepdims=False)
        return jnp.concatenate([g, u], axis=1)

    def down_block(k):
        return lax.dynamic_index_in_dim(
            down_weight, lax.rem(me + k, local), 0, keepdims=False
        )

    w_in = [in_block(0)] + [beside(in_block(k), k) for k in range(1, local)]

    rt = routing.T
    expert = jnp.arange(ep, dtype=jnp.int32) * local + me
    hit = rt[:, None, :] == expert[None, :, None]
    named = jnp.any(hit, axis=0)
    scale = jnp.sum(jnp.where(hit, gate_fixed.T[:, None, :], 0), axis=0)
    t = jnp.arange(rows)
    before = (t[:, None] < t[None, :]).astype(BF16)
    position = jnp.dot(named.astype(BF16), before, preferred_element_type=F32)
    slot = jnp.arange(capacity).astype(F32)[None, :, None]
    pick = named[:, None, :] & (position[:, None, :] == slot)
    place = pick.astype(BF16).reshape(slots, rows)
    factor = scale.astype(F32) / 65536.0
    mix = jnp.where(pick, factor[:, None, :], 0.0).reshape(slots, rows)

    outgoing = rows_dot(place, xt).astype(BF16)
    sent = [down_block(k) for k in range(1, local)]
    outgoing, sent = lax.optimization_barrier((outgoing, sent))
    x = exchange(outgoing.reshape(ep, capacity, -1), "ep")
    w_down = [down_block(0)] + [beside(b, k + 1) for k, b in enumerate(sent)]
    w_down = jnp.concatenate(w_down, axis=0)

    x = x.reshape(ring, chunk, -1)
    w_in = jnp.concatenate(w_in, axis=0)

    def term(k):
        rows_of = lax.dynamic_index_in_dim(x, chunk_at[k % ring], 0, keepdims=False)
        return jnp.dot(rows_of, w_in, preferred_element_type=F32)

    steps = ring // 2
    ahead = ship(term(steps).astype(BF16), 1)
    behind = ship(term(1 - steps).astype(BF16), -1)
    for k in range(steps - 1, 0, -1):
        ahead = ship((term(k) + ahead.astype(F32)).astype(BF16), 1)
        if k > 1:
            behind = ship((term(1 - k) + behind.astype(F32)).astype(BF16), -1)
    acts = term(0) + ahead.astype(F32) + behind.astype(F32)
    own = (jax.nn.silu(acts[:, :units]) * acts[:, units:]).astype(BF16)

    hidden = jnp.zeros((ring, chunk, units), BF16)

    def put(hidden, arrived, k):
        return lax.dynamic_update_index_in_dim(hidden, arrived, chunk_at[k % ring], 0)

    ahead = behind = own
    hidden = put(hidden, own, 0)
    for k in range(1, steps + 1):
        ahead = ship(ahead, 1)
        hidden = put(hidden, ahead, -k)
        if k < steps:
            behind = ship(behind, -1)
            hidden = put(hidden, behind, k)
    result = rows_dot(hidden.reshape(slots, units), w_down)
    back = exchange(result.reshape(ep, capacity, -1), "ep").reshape(slots, -1)

    mixed = lax.dot_general(
        back,
        mix,
        (((0,), (0,)), ((), ())),
        precision=lax.Precision.HIGHEST,
        preferred_element_type=F32,
    ).reshape(local, share, rows)
    parts = exchange(jnp.stack(picked(mixed, order)), "tp", near)
    return jnp.sum(parts, axis=0).astype(BF16).T


def solution(mesh):
    in_specs = (
        P("ep", "tp"),
        P("ep", None),
        P("ep", None),
        P("ep", "tp", None),
        P("ep", "tp", None),
        P("ep", "tp", None),
    )
    return jax.shard_map(
        layer, mesh=mesh, in_specs=in_specs, out_specs=P("ep", "tp"), check_vma=False
    )
```

```python
import jax
import jax.numpy as jnp
from jax import lax
from jax.sharding import PartitionSpec as P

F32 = jnp.float32
BF16 = jnp.bfloat16


def exchange(x, axis, groups=None):
    return lax.all_to_all(
        x, axis, split_axis=0, concat_axis=0, tiled=True, axis_index_groups=groups
    )


def picked(x, places):
    return [lax.dynamic_index_in_dim(x, i, 0, keepdims=False) for i in places]


def rows_dot(a, b):
    return lax.dot_general(a, b, (((1,), (1,)), ((), ())), preferred_element_type=F32)


def layer(tokens, routing, gate_fixed, gate_weight, up_weight, down_weight):
    ep = lax.axis_size("ep")
    tp = lax.axis_size("tp")
    local, share, units = gate_weight.shape
    rows, top = routing.shape
    capacity = max(2, rows * top * 2 // (local * ep))
    ring = tp // local
    slots = ep * capacity
    chunk = slots // ring
    near = [[p * local + r for r in range(local)] for p in range(ring)]
    z = lax.axis_index("tp")
    me = lax.rem(z, local)
    here = lax.div(z, local)

    def sign_of(r):
        return 1 if r < local // 2 else -1

    sign = jnp.where(me < local // 2, 1, -1)

    def ship(x, side):
        pairs = [
            (p * local + r, (p + side * sign_of(r)) % ring * local + r)
            for p in range(ring)
            for r in range(local)
        ]
        return lax.ppermute(x, "tp", pairs)

    def beside(x, k):
        return lax.ppermute(
            x, "tp", [(g[i], g[(i + k) % local]) for g in near for i in range(local)]
        )

    chunk_at = [lax.rem(here + k * sign + ring, ring) for k in range(ring)]

    xt = exchange(jnp.broadcast_to(tokens.T[None], (local, share, rows)), "tp", near)
    order = [lax.rem(me - k + local, local) for k in range(local)]
    xt = jnp.concatenate(picked(xt, order), axis=0)

    def in_block(k):
        e = lax.rem(me + k, local)
        g = lax.dynamic_index_in_dim(gate_weight, e, 0, keepdims=False)
        u = lax.dynamic_index_in_dim(up_weight, e, 0, keepdims=False)
        d = lax.dynamic_index_in_dim(down_weight, e, 0, keepdims=False)
        return jnp.concatenate([g, u, d], axis=1)

    blocks = [in_block(0)] + [beside(in_block(k), k) for k in range(1, local)]
    w_in = jnp.concatenate([b[:, : 2 * units] for b in blocks], axis=0)
    w_down = jnp.concatenate([b[:, 2 * units :] for b in blocks], axis=0)

    rt = routing.T
    expert = jnp.arange(ep, dtype=jnp.int32) * local + me
    hit = rt[:, None, :] == expert[None, :, None]
    named = jnp.any(hit, axis=0)
    scale = jnp.sum(jnp.where(hit, gate_fixed.T[:, None, :], 0), axis=0)
    t = jnp.arange(rows)
    before = (t[:, None] < t[None, :]).astype(BF16)
    position = jnp.dot(named.astype(BF16), before, preferred_element_type=F32)
    slot = jnp.arange(capacity).astype(F32)[None, :, None]
    pick = named[:, None, :] & (position[:, None, :] == slot)
    place = pick.astype(BF16).reshape(slots, rows)
    factor = scale.astype(F32) / 65536.0
    mix = jnp.where(pick, factor[:, None, :], 0.0).reshape(slots, rows)

    outgoing = rows_dot(place, xt).astype(BF16)
    x = exchange(outgoing.reshape(ep, capacity, -1), "ep")
    x = x.reshape(ring, chunk, -1)

    def term(k):
        rows_of = lax.dynamic_index_in_dim(x, chunk_at[k % ring], 0, keepdims=False)
        return jnp.dot(rows_of, w_in, preferred_element_type=F32)

    steps = ring // 2
    ahead = ship(term(steps).astype(BF16), 1)
    behind = ship(term(1 - steps).astype(BF16), -1)
    for k in range(steps - 1, 0, -1):
        ahead = ship((term(k) + ahead.astype(F32)).astype(BF16), 1)
        if k > 1:
            behind = ship((term(1 - k) + behind.astype(F32)).astype(BF16), -1)
    acts = term(0) + ahead.astype(F32) + behind.astype(F32)
    own = (jax.nn.silu(acts[:, :units]) * acts[:, units:]).astype(BF16)

    hidden = jnp.zeros((ring, chunk, units), BF16)

    def put(hidden, arrived, k):
        return lax.dynamic_update_index_in_dim(hidden, arrived, chunk_at[k % ring], 0)

    ahead = behind = own
    hidden = put(hidden, lax.optimization_barrier(own), 0)
    for k in range(1, steps + 1):
        ahead = ship(ahead, 1)
        hidden = put(hidden, ahead, -k)
        if k < steps:
            behind = ship(behind, -1)
            hidden = put(hidden, behind, k)
    result = rows_dot(hidden.reshape(slots, units), w_down)
    back = exchange(result.reshape(ep, capacity, -1), "ep").reshape(slots, -1)

    mixed = lax.dot_general(
        back,
        mix,
        (((0,), (0,)), ((), ())),
        precision=lax.Precision.HIGHEST,
        preferred_element_type=F32,
    ).reshape(local, share, rows)
    parts = exchange(jnp.stack(picked(mixed, order)), "tp", near)
    return jnp.sum(parts, axis=0).astype(BF16).T


def solution(mesh):
    in_specs = (
        P("ep", "tp"),
        P("ep", None),
        P("ep", None),
        P("ep", "tp", None),
        P("ep", "tp", None),
        P("ep", "tp", None),
    )
    return jax.shard_map(
        layer, mesh=mesh, in_specs=in_specs, out_specs=P("ep", "tp"), check_vma=False
    )
```

```python
import jax
import jax.numpy as jnp
from jax import lax
from jax.sharding import PartitionSpec as P

F32 = jnp.float32
BF16 = jnp.bfloat16


def exchange(x, axis, groups=None):
    return lax.all_to_all(
        x, axis, split_axis=0, concat_axis=0, tiled=True, axis_index_groups=groups
    )


def picked(x, places):
    return [lax.dynamic_index_in_dim(x, i, 0, keepdims=False) for i in places]


def rows_dot(a, b):
    return lax.dot_general(a, b, (((1,), (1,)), ((), ())), preferred_element_type=F32)


def layer(tokens, routing, gate_fixed, gate_weight, up_weight, down_weight):
    ep = lax.axis_size("ep")
    tp = lax.axis_size("tp")
    local, share, units = gate_weight.shape
    rows, top = routing.shape
    capacity = max(2, rows * top * 2 // (local * ep))
    ring = tp // local
    slots = ep * capacity
    chunk = slots // ring
    near = [[p * local + r for r in range(local)] for p in range(ring)]
    z = lax.axis_index("tp")
    me = lax.rem(z, local)
    here = lax.div(z, local)

    def sign_of(r):
        return 1 if r < local // 2 else -1

    sign = jnp.where(me < local // 2, 1, -1)

    def ship(x, side):
        pairs = [
            (p * local + r, (p + side * sign_of(r)) % ring * local + r)
            for p in range(ring)
            for r in range(local)
        ]
        return lax.ppermute(x, "tp", pairs)

    def beside(x, k):
        return lax.ppermute(
            x, "tp", [(g[i], g[(i + k) % local]) for g in near for i in range(local)]
        )

    chunk_at = [lax.rem(here + k * sign + ring, ring) for k in range(ring)]

    xt = exchange(jnp.broadcast_to(tokens.T[None], (local, share, rows)), "tp", near)
    order = [lax.rem(me - k + local, local) for k in range(local)]
    xt = jnp.concatenate(picked(xt, order), axis=0)

    def in_block(k):
        e = lax.rem(me + k, local)
        g = lax.dynamic_index_in_dim(gate_weight, e, 0, keepdims=False)
        u = lax.dynamic_index_in_dim(up_weight, e, 0, keepdims=False)
        d = lax.dynamic_index_in_dim(down_weight, e, 0, keepdims=False)
        return jnp.concatenate([g, u, d], axis=1)

    blocks = [in_block(0)] + [beside(in_block(k), k) for k in range(1, local)]
    w_in = jnp.concatenate([b[:, : 2 * units] for b in blocks], axis=0)
    w_down = jnp.concatenate([b[:, 2 * units :] for b in blocks], axis=0)

    rt = routing.T
    expert = jnp.arange(ep, dtype=jnp.int32) * local + me
    hit = rt[:, None, :] == expert[None, :, None]
    named = jnp.any(hit, axis=0)
    scale = jnp.sum(jnp.where(hit, gate_fixed.T[:, None, :], 0), axis=0)
    t = jnp.arange(rows)
    before = (t[:, None] < t[None, :]).astype(BF16)
    position = jnp.dot(named.astype(BF16), before, preferred_element_type=F32)
    slot = jnp.arange(capacity).astype(F32)[None, :, None]
    pick = named[:, None, :] & (position[:, None, :] == slot)
    place = pick.astype(BF16).reshape(slots, rows)
    factor = scale.astype(F32) / 65536.0
    mix = jnp.where(pick, factor[:, None, :], 0.0).reshape(slots, rows)

    outgoing = rows_dot(place, xt).astype(BF16)
    x = exchange(outgoing.reshape(ep, capacity, -1), "ep")
    x = x.reshape(ring, chunk, -1)

    def term(k):
        rows_of = lax.dynamic_index_in_dim(x, chunk_at[k % ring], 0, keepdims=False)
        return jnp.dot(rows_of, w_in, preferred_element_type=F32)

    steps = ring // 2
    ahead = ship(term(steps).astype(BF16), 1)
    early = [3, -2, 2, -1, 1]
    made = [term(k) for k in early]
    first = term(1 - steps).astype(BF16)
    first, made = lax.optimization_barrier((first, made))
    made = dict(zip(early, made))
    made[0] = term(0)
    behind = ship(first, -1)
    for k in range(steps - 1, 0, -1):
        ahead = ship((made[k] + ahead.astype(F32)).astype(BF16), 1)
        if k > 1:
            behind = ship((made[1 - k] + behind.astype(F32)).astype(BF16), -1)
    acts = made[0] + ahead.astype(F32) + behind.astype(F32)
    own = (jax.nn.silu(acts[:, :units]) * acts[:, units:]).astype(BF16)

    hidden = jnp.zeros((ring, chunk, units), BF16)

    def put(hidden, arrived, k):
        return lax.dynamic_update_index_in_dim(hidden, arrived, chunk_at[k % ring], 0)

    ahead = behind = own
    hidden = put(hidden, lax.optimization_barrier(own), 0)
    for k in range(1, steps + 1):
        ahead = ship(ahead, 1)
        hidden = put(hidden, ahead, -k)
        if k < steps:
            behind = ship(behind, -1)
            hidden = put(hidden, behind, k)
    result = rows_dot(hidden.reshape(slots, units), w_down)
    back = exchange(result.reshape(ep, capacity, -1), "ep").reshape(slots, -1)

    mixed = lax.dot_general(
        back,
        mix,
        (((0,), (0,)), ((), ())),
        precision=lax.Precision.HIGHEST,
        preferred_element_type=F32,
    ).reshape(local, share, rows)
    parts = exchange(jnp.stack(picked(mixed, order)), "tp", near)
    return jnp.sum(parts, axis=0).astype(BF16).T


def solution(mesh):
    in_specs = (
        P("ep", "tp"),
        P("ep", None),
        P("ep", None),
        P("ep", "tp", None),
        P("ep", "tp", None),
        P("ep", "tp", None),
    )
    return jax.shard_map(
        layer, mesh=mesh, in_specs=in_specs, out_specs=P("ep", "tp"), check_vma=False
    )
```

```python
import jax
import jax.numpy as jnp
from jax import lax
from jax.sharding import PartitionSpec as P

F32 = jnp.float32
BF16 = jnp.bfloat16


def exchange(x, axis, groups=None):
    return lax.all_to_all(
        x, axis, split_axis=0, concat_axis=0, tiled=True, axis_index_groups=groups
    )


def picked(x, places):
    return [lax.dynamic_index_in_dim(x, i, 0, keepdims=False) for i in places]


def rows_dot(a, b):
    return lax.dot_general(a, b, (((1,), (1,)), ((), ())), preferred_element_type=F32)


def layer(tokens, routing, gate_fixed, gate_weight, up_weight, down_weight):
    ep = lax.axis_size("ep")
    tp = lax.axis_size("tp")
    local, share, units = gate_weight.shape
    rows, top = routing.shape
    capacity = max(2, rows * top * 2 // (local * ep))
    ring = tp // local
    slots = ep * capacity
    chunk = slots // ring
    near = [[p * local + r for r in range(local)] for p in range(ring)]
    z = lax.axis_index("tp")
    me = lax.rem(z, local)
    here = lax.div(z, local)

    def sign_of(r):
        return 1 if r < local // 2 else -1

    sign = jnp.where(me < local // 2, 1, -1)

    def ship(x, side):
        pairs = [
            (p * local + r, (p + side * sign_of(r)) % ring * local + r)
            for p in range(ring)
            for r in range(local)
        ]
        return lax.ppermute(x, "tp", pairs)

    def beside(x, k):
        return lax.ppermute(
            x, "tp", [(g[i], g[(i + k) % local]) for g in near for i in range(local)]
        )

    chunk_at = [lax.rem(here + k * sign + ring, ring) for k in range(ring)]

    xt = exchange(jnp.broadcast_to(tokens.T[None], (local, share, rows)), "tp", near)
    order = [lax.rem(me - k + local, local) for k in range(local)]
    xt = jnp.concatenate(picked(xt, order), axis=0)

    def in_block(k):
        e = lax.rem(me + k, local)
        g = lax.dynamic_index_in_dim(gate_weight, e, 0, keepdims=False)
        u = lax.dynamic_index_in_dim(up_weight, e, 0, keepdims=False)
        return jnp.concatenate([g, u], axis=1)

    def down_block(k):
        return lax.dynamic_index_in_dim(
            down_weight, lax.rem(me + k, local), 0, keepdims=False
        )

    w_in = [in_block(0)] + [beside(in_block(k), k) for k in range(1, local)]
    w_in = jnp.concatenate(w_in, axis=0)

    rt = routing.T
    expert = jnp.arange(ep, dtype=jnp.int32) * local + me
    hit = rt[:, None, :] == expert[None, :, None]
    named = jnp.any(hit, axis=0)
    scale = jnp.sum(jnp.where(hit, gate_fixed.T[:, None, :], 0), axis=0)
    t = jnp.arange(rows)
    before = (t[:, None] < t[None, :]).astype(BF16)
    position = jnp.dot(named.astype(BF16), before, preferred_element_type=F32)
    slot = jnp.arange(capacity).astype(F32)[None, :, None]
    pick = named[:, None, :] & (position[:, None, :] == slot)
    place = pick.astype(BF16).reshape(slots, rows)
    factor = scale.astype(F32) / 65536.0
    mix = jnp.where(pick, factor[:, None, :], 0.0).reshape(slots, rows)

    outgoing = rows_dot(place, xt).astype(BF16)
    sent = [down_block(k) for k in range(1, local)]
    outgoing, sent = lax.optimization_barrier((outgoing, sent))
    x = exchange(outgoing.reshape(ep, capacity, -1), "ep")
    w_down = [down_block(0)] + [beside(b, k + 1) for k, b in enumerate(sent)]
    w_down = jnp.concatenate(w_down, axis=0)

    x = x.reshape(ring, chunk, -1)

    def term(k):
        rows_of = lax.dynamic_index_in_dim(x, chunk_at[k % ring], 0, keepdims=False)
        return jnp.dot(rows_of, w_in, preferred_element_type=F32)

    steps = ring // 2
    ahead = ship(term(steps).astype(BF16), 1)
    early = [3, -2, 2, -1, 1]
    made = [term(k) for k in early]
    first = term(1 - steps).astype(BF16)
    first, made = lax.optimization_barrier((first, made))
    made = dict(zip(early, made))
    made[0] = term(0)
    behind = ship(first, -1)
    for k in range(steps - 1, 0, -1):
        ahead = ship((made[k] + ahead.astype(F32)).astype(BF16), 1)
        if k > 1:
            behind = ship((made[1 - k] + behind.astype(F32)).astype(BF16), -1)
    acts = made[0] + ahead.astype(F32) + behind.astype(F32)
    own = (jax.nn.silu(acts[:, :units]) * acts[:, units:]).astype(BF16)

    hidden = jnp.zeros((ring, chunk, units), BF16)

    def put(hidden, arrived, k):
        return lax.dynamic_update_index_in_dim(hidden, arrived, chunk_at[k % ring], 0)

    ahead = behind = own
    hidden = put(hidden, lax.optimization_barrier(own), 0)
    for k in range(1, steps + 1):
        ahead = ship(ahead, 1)
        hidden = put(hidden, ahead, -k)
        if k < steps:
            behind = ship(behind, -1)
            hidden = put(hidden, behind, k)
    result = rows_dot(hidden.reshape(slots, units), w_down)
    back = exchange(result.reshape(ep, capacity, -1), "ep").reshape(slots, -1)

    mixed = lax.dot_general(
        back,
        mix,
        (((0,), (0,)), ((), ())),
        precision=lax.Precision.HIGHEST,
        preferred_element_type=F32,
    ).reshape(local, share, rows)
    parts = exchange(jnp.stack(picked(mixed, order)), "tp", near)
    return jnp.sum(parts, axis=0).astype(BF16).T


def solution(mesh):
    in_specs = (
        P("ep", "tp"),
        P("ep", None),
        P("ep", None),
        P("ep", "tp", None),
        P("ep", "tp", None),
        P("ep", "tp", None),
    )
    return jax.shard_map(
        layer, mesh=mesh, in_specs=in_specs, out_specs=P("ep", "tp"), check_vma=False
    )
```

```python
import jax
import jax.numpy as jnp
from jax import lax
from jax.sharding import PartitionSpec as P

F32 = jnp.float32
BF16 = jnp.bfloat16


def exchange(x, axis, groups=None):
    return lax.all_to_all(
        x, axis, split_axis=0, concat_axis=0, tiled=True, axis_index_groups=groups
    )


def picked(x, places):
    return [lax.dynamic_index_in_dim(x, i, 0, keepdims=False) for i in places]


def rows_dot(a, b):
    return lax.dot_general(a, b, (((1,), (1,)), ((), ())), preferred_element_type=F32)


def layer(tokens, routing, gate_fixed, gate_weight, up_weight, down_weight):
    ep = lax.axis_size("ep")
    tp = lax.axis_size("tp")
    local, share, units = gate_weight.shape
    rows, top = routing.shape
    capacity = max(2, rows * top * 2 // (local * ep))
    ring = tp // local
    slots = ep * capacity
    chunk = slots // ring
    near = [[p * local + r for r in range(local)] for p in range(ring)]
    z = lax.axis_index("tp")
    me = lax.rem(z, local)
    here = lax.div(z, local)

    def sign_of(r):
        return 1 if r % 2 == 0 else -1

    sign = 1 - 2 * lax.rem(me, 2)

    def ship(x, side):
        pairs = [
            (p * local + r, (p + side * sign_of(r)) % ring * local + r)
            for p in range(ring)
            for r in range(local)
        ]
        return lax.ppermute(x, "tp", pairs)

    def beside(x, k):
        return lax.ppermute(
            x, "tp", [(g[i], g[(i + k) % local]) for g in near for i in range(local)]
        )

    chunk_at = [lax.rem(here + k * sign + ring, ring) for k in range(ring)]

    xt = exchange(jnp.broadcast_to(tokens.T[None], (local, share, rows)), "tp", near)
    order = [lax.rem(me - k + local, local) for k in range(local)]
    xt = jnp.concatenate(picked(xt, order), axis=0)

    def in_block(k):
        e = lax.rem(me + k, local)
        g = lax.dynamic_index_in_dim(gate_weight, e, 0, keepdims=False)
        u = lax.dynamic_index_in_dim(up_weight, e, 0, keepdims=False)
        return jnp.concatenate([g, u], axis=1)

    def down_block(k):
        return lax.dynamic_index_in_dim(
            down_weight, lax.rem(me + k, local), 0, keepdims=False
        )

    w_in = [in_block(0)] + [beside(in_block(k), k) for k in range(1, local)]
    w_in = jnp.concatenate(w_in, axis=0)

    rt = routing.T
    expert = jnp.arange(ep, dtype=jnp.int32) * local + me
    hit = rt[:, None, :] == expert[None, :, None]
    named = jnp.any(hit, axis=0)
    scale = jnp.sum(jnp.where(hit, gate_fixed.T[:, None, :], 0), axis=0)
    t = jnp.arange(rows)
    before = (t[:, None] < t[None, :]).astype(BF16)
    position = jnp.dot(named.astype(BF16), before, preferred_element_type=F32)
    slot = jnp.arange(capacity).astype(F32)[None, :, None]
    pick = named[:, None, :] & (position[:, None, :] == slot)
    place = pick.astype(BF16).reshape(slots, rows)
    factor = scale.astype(F32) / 65536.0
    mix = jnp.where(pick, factor[:, None, :], 0.0).reshape(slots, rows)

    outgoing = rows_dot(place, xt).astype(BF16)
    sent = [down_block(k) for k in range(1, local)]
    outgoing, sent = lax.optimization_barrier((outgoing, sent))
    x = exchange(outgoing.reshape(ep, capacity, -1), "ep")
    w_down = [down_block(0)] + [beside(b, k + 1) for k, b in enumerate(sent)]
    w_down = jnp.concatenate(w_down, axis=0)

    x = x.reshape(ring, chunk, -1)

    def term(k):
        rows_of = lax.dynamic_index_in_dim(x, chunk_at[k % ring], 0, keepdims=False)
        return jnp.dot(rows_of, w_in, preferred_element_type=F32)

    steps = ring // 2
    ahead = ship(term(steps).astype(BF16), 1)
    early = [3, -2, 2, -1, 1, 0]
    made = [term(k) for k in early]
    first = term(1 - steps).astype(BF16)
    first, made = lax.optimization_barrier((first, made))
    made = dict(zip(early, made))
    behind = ship(first, -1)
    for k in range(steps - 1, 0, -1):
        ahead = ship((made[k] + ahead.astype(F32)).astype(BF16), 1)
        if k > 1:
            behind = ship((made[1 - k] + behind.astype(F32)).astype(BF16), -1)
    acts = made[0] + ahead.astype(F32) + behind.astype(F32)
    own = (jax.nn.silu(acts[:, :units]) * acts[:, units:]).astype(BF16)

    hidden = jnp.zeros((ring, chunk, units), BF16)

    def put(hidden, arrived, k):
        return lax.dynamic_update_index_in_dim(hidden, arrived, chunk_at[k % ring], 0)

    ahead = behind = own
    hidden = put(hidden, lax.optimization_barrier(own), 0)
    for k in range(1, steps + 1):
        ahead = ship(ahead, 1)
        hidden = put(hidden, ahead, -k)
        if k < steps:
            behind = ship(behind, -1)
            hidden = put(hidden, behind, k)
    result = rows_dot(hidden.reshape(slots, units), w_down)
    back = exchange(result.reshape(ep, capacity, -1), "ep").reshape(slots, -1)

    mixed = lax.dot_general(
        back,
        mix,
        (((0,), (0,)), ((), ())),
        precision=lax.Precision.HIGHEST,
        preferred_element_type=F32,
    ).reshape(local, share, rows)
    parts = exchange(jnp.stack(picked(mixed, order)), "tp", near)
    return jnp.sum(parts, axis=0).astype(BF16).T


def solution(mesh):
    in_specs = (
        P("ep", "tp"),
        P("ep", None),
        P("ep", None),
        P("ep", "tp", None),
        P("ep", "tp", None),
        P("ep", "tp", None),
    )
    return jax.shard_map(
        layer, mesh=mesh, in_specs=in_specs, out_specs=P("ep", "tp"), check_vma=False
    )
```
